32 devices in a mesh: node: 8 (over z, x), local: 4 (over y, core).
Axes of the slice: x: 2, y: 2, z: 4, core: 2. Of those that a mesh axis runs over, the one named last changes fastest.
Arguments:
- tokens: bfloat16 [2048, 5120], P(('node', 'local')), may hold values from -6 to 6
- node_ids: int32 [2048, 3], P(('node', 'local')), may hold values from 0 to 7, as said below
- expert_ids: int32 [2048, 6], P(('node', 'local')), may hold values from 0 to 23, as said below
- gate_weights: bfloat16 [2048, 6], P(('node', 'local')), may hold values from 0.049804688 to 1
- up_weight: bfloat16 [24, 5120, 1536], P('node', None, 'local'), may hold values from -0.078125 to 0.078125
- down_weight: bfloat16 [24, 1536, 5120], P('node', 'local'), may hold values from -0.15625 to 0.15625
Outputs:
- routed_out: bfloat16 [2048, 5120], P(('node', 'local'))
The draws below stay inside these ranges and needn't reach their ends.
Inputs may be any that keep to these rules, and one draw needn't show every extreme that they name: `node_ids`: each token names 3 different nodes; the 64 tokens of one device name every node exactly 24 times. Node m holds experts 3 * m to 3 * m + 2. For each j, expert_ids[t, 2 * j] and expert_ids[t, 2 * j + 1] are two different experts of node node_ids[t, j].
All inputs are finite; a program needn't handle non-finite values.
Results may differ from the reference program's by a relative error of at most 0.012.
Values may be sent and summed in bfloat16 or wider, within the bound.
A program may use at most 192 MiB of HBM per device.

```python
import math
import jax
import jax.numpy as jnp
from jax import lax

D = 5120
FF = 1536
EXP_NODE = 3
TOPK = 6
NODES_SEL = 3
TOK_DEV = 64
TOKENS = 2048
EXPERTS = 24
CAP = 24
N_NODE = 8
N_LOCAL = 4


def routing_tables(key):
    blocks_total = TOKENS // TOK_DEV
    node_total = EXPERTS // EXP_NODE
    base_key = jax.random.fold_in(key, 11)

    def one_block(block_key):
        key_order, key_tokens, key_skip = jax.random.split(block_key, 3)
        node_order = jax.random.permutation(key_order, node_total).astype(jnp.int32)
        cycled = node_order[jnp.arange(NODES_SEL * TOK_DEV, dtype=jnp.int32) % node_total]
        triples = cycled.reshape(TOK_DEV, NODES_SEL)
        shuffled = triples[jax.random.permutation(key_tokens, TOK_DEV)]
        skipped = jax.random.randint(key_skip, (TOK_DEV, NODES_SEL), 0, EXP_NODE).astype(jnp.int32)
        return (shuffled, skipped)
    node_table, skip_table = jax.vmap(one_block)(jax.random.split(base_key, blocks_total))
    return (node_table.reshape(TOKENS, NODES_SEL), skip_table.reshape(TOKENS, NODES_SEL))


def draw_node_ids(key, part):
    node_table, skip_table = routing_tables(key)
    return node_table.astype(jnp.int32)


def draw_expert_ids(key, part):
    node_table, skip_table = routing_tables(key)
    first_pick = (skip_table + 1) % EXP_NODE
    second = (skip_table + 2) % EXP_NODE
    paired = jnp.stack([node_table * EXP_NODE + first_pick, node_table * EXP_NODE + second], axis=2)
    return paired.reshape(TOKENS, TOPK).astype(jnp.int32)


def shard_levels(stream_key, extent, cuts, low, largest):
    loudness = 1.0
    for axis_at, parts in cuts:
        heights = jax.random.uniform(jax.random.fold_in(jax.random.fold_in(stream_key, 6), axis_at), (parts,), jnp.float32, low / len(cuts), largest / len(cuts))
        loudness = loudness * jnp.repeat(jnp.exp(heights), extent[axis_at] // parts).reshape((-1,) + (1,) * (len(extent) - 1 - axis_at))
    return loudness


def bell_draw(key, dims, width, bound, pieces=(), kind=jnp.bfloat16):
    factor_of = shard_levels(key, dims, pieces, -0.22, 0.18) if pieces else 1.0
    values = jax.random.normal(key, dims, jnp.float32) * width * factor_of
    return jnp.minimum(jnp.maximum(values, -bound), bound).astype(kind)


def setup_inputs(seed: int = 0) -> dict:
    key_list = jax.random.split(jax.random.key(seed), 7)
    return {
        "tokens": bell_draw(key_list[0], (TOKENS, D), 1.0, 6.0, ((0, 32),)),
        "node_ids": draw_node_ids(jax.random.fold_in(key_list[6], 71), 0),
        "expert_ids": draw_expert_ids(jax.random.fold_in(key_list[6], 71), 0),
        "gate_weights": jnp.clip(jnp.exp(math.log(1.0) - 2.9996462 * jax.random.uniform(key_list[3], (TOKENS, TOPK), jnp.float32) ** shard_levels(key_list[3], (TOKENS, TOPK), ((0, 32),), -0.2, 0.2)), 0.049804688, 1.0).astype(jnp.bfloat16),
        "up_weight": bell_draw(key_list[4], (EXPERTS, D, FF), D ** -0.5, 0.078125, ((0, 8), (2, 4))),
        "down_weight": bell_draw(key_list[5], (EXPERTS, FF, D), FF ** -0.5, 0.15625, ((0, 8), (1, 4))),
    }


def reference(tokens, node_ids, expert_ids, gate_weights, up_weight, down_weight):
    row_total = N_NODE * N_LOCAL * CAP
    shard_size = FF // N_LOCAL

    def per_node(running, node_id):
        chosen = jnp.any(node_ids == node_id, axis=1)
        row_index = jnp.nonzero(chosen, size=row_total, fill_value=0)[0].astype(jnp.int32)
        picked = tokens[row_index]
        row_experts = expert_ids[row_index]
        row_gates = gate_weights[row_index].astype(jnp.float32)
        contrib = jnp.zeros((row_total, D), jnp.float32)
        for shard_index in range(N_LOCAL):
            partial_value = jnp.zeros((row_total, D), jnp.float32)
            for expert_slot in range(EXP_NODE):
                expert = node_id * EXP_NODE + expert_slot
                weight = jnp.sum(jnp.where(row_experts == expert, row_gates, jnp.float32(0.0)), axis=1)
                up_full = lax.dynamic_index_in_dim(up_weight, expert, 0, keepdims=False)
                down_full = lax.dynamic_index_in_dim(down_weight, expert, 0, keepdims=False)
                up_slice = up_full[:, shard_index * shard_size:(shard_index + 1) * shard_size]
                down_slice = down_full[shard_index * shard_size:(shard_index + 1) * shard_size, :]
                lifted = jnp.dot(picked, up_slice, preferred_element_type=jnp.float32)
                scaled = (jax.nn.silu(lifted) * weight[:, None]).astype(jnp.bfloat16)
                partial_value = partial_value + jnp.dot(scaled, down_slice, preferred_element_type=jnp.float32)
            contrib = contrib + partial_value.astype(jnp.bfloat16).astype(jnp.float32)
        running = running.at[row_index].add(contrib.astype(jnp.bfloat16).astype(jnp.float32))
        return running, None

    final_sum, unused = lax.scan(per_node, jnp.zeros((TOKENS, D), jnp.float32), jnp.arange(N_NODE, dtype=jnp.int32))
    return final_sum.astype(jnp.bfloat16)
```

```python
import functools

import jax
import jax.numpy as jnp
from jax import lax
from jax.experimental import pallas as pl
from jax.experimental.pallas import tpu as pltpu
from jax.sharding import PartitionSpec as P

GROUPS = 4
LANES = 128
MESH = pl.DeviceIdType.MESH


def partner(index, step, bits):
    total = 0
    for b in range(bits):
        w = 1 << b
        total = total + ((index // w + step // w) % 2) * w
    return total


def dot(a, b):
    return jnp.dot(a, b, preferred_element_type=jnp.float32)


def kernel(
    cfg,
    tok_ref, nid_ref, eid_ref, gate_ref, up_hbm, down_hbm,
    out_ref,
    up, down, toks, ext, ext_own, packed, rx, px, hid, p_own, p_oth, pr, yr, back, place, final,
    w_sem, x_send, x_recv, a_send, a_recv, y_send, y_recv, d_send, d_recv,
    e_send, e_recv, c_send, c_recv, b_send, b_recv, f_send, f_recv,
):
    n, bits, cap, blk, rows, half, width, per_node, unit, chunk = cfg
    gs = n // GROUPS
    gh = gs * blk
    quota = n * blk
    node = lax.axis_index("node")
    loc = lax.axis_index("local")
    hi, lo = loc // 2, loc % 2
    lo_peer = (node, hi * 2 + (1 - lo))
    hi_peer = (node, (1 - hi) * 2 + lo)

    def remote(src, dst, ssem, rsem, dev):
        return pltpu.make_async_remote_copy(
            src_ref=src, dst_ref=dst, send_sem=ssem, recv_sem=rsem,
            device_id=dev, device_id_type=MESH,
        )

    up_copy = pltpu.make_async_copy(up_hbm, up, w_sem.at[0])
    down_copy = pltpu.make_async_copy(down_hbm, down, w_sem.at[1])
    up_copy.start()
    down_copy.start()

    barrier = pltpu.get_barrier_semaphore()
    for s in range(1, n):
        pl.semaphore_signal(barrier, inc=1, device_id=(partner(node, s, bits), loc), device_id_type=MESH)
    pl.semaphore_signal(barrier, inc=1, device_id=lo_peer, device_id_type=MESH)
    pl.semaphore_signal(barrier, inc=1, device_id=hi_peer, device_id_type=MESH)

    k_sel = nid_ref.shape[1]
    k_top = eid_ref.shape[1]
    lane_r = lax.broadcasted_iota(jnp.int32, (rows, LANES), 1)
    facts = jnp.zeros((rows, LANES), jnp.float32)
    nid = nid_ref[...].astype(jnp.float32)
    eid = eid_ref[...].astype(jnp.float32)
    gat = gate_ref[...].astype(jnp.float32)
    for j in range(k_sel):
        facts = jnp.where(lane_r == j, nid[:, j : j + 1], facts)
    for j in range(k_top):
        facts = jnp.where(lane_r == k_sel + j, eid[:, j : j + 1], facts)
        facts = jnp.where(lane_r == k_sel + k_top + j, gat[:, j : j + 1], facts)
    mine = pl.ds(pl.multiple_of(lo * rows, rows), rows)
    ext_own[...] = facts.astype(jnp.bfloat16)
    my_cols = pl.ds(pl.multiple_of(lo * half, LANES), half)
    peer_cols = pl.ds(pl.multiple_of((1 - lo) * half, LANES), half)

    pl.semaphore_wait(barrier, n + 1)
    ext_copy = remote(ext_own, ext.at[mine], x_send.at[0], x_recv.at[0], lo_peer)
    ext_copy.start()
    tok_copy = remote(tok_ref.at[:, peer_cols], toks.at[mine], x_send.at[1], x_recv.at[1], lo_peer)
    tok_copy.start()
    ext[mine, :] = facts.astype(jnp.bfloat16)
    toks[mine, :] = tok_ref[:, my_cols]
    ext_copy.wait()

    both = 2 * rows
    f = ext[...].astype(jnp.float32)
    lane = lax.broadcasted_iota(jnp.int32, (both, LANES), 1)
    row = lax.broadcasted_iota(jnp.int32, (both, LANES), 0)
    nlane = jnp.where(lane < n, jnp.bitwise_xor(lane, node), -1).astype(jnp.float32)
    picked = jnp.zeros((both, LANES), jnp.float32)
    for j in range(k_sel):
        picked = picked + jnp.where(f[:, j : j + 1] == nlane, 1.0, 0.0)
    tr = lax.broadcasted_iota(jnp.int32, (both, both), 0)
    tc = lax.broadcasted_iota(jnp.int32, (both, both), 1)
    earlier = jnp.where((tc < tr) & ((tc >= rows) == (tr >= rows)), 1.0, 0.0).astype(jnp.bfloat16)
    rank = dot(earlier, picked.astype(jnp.bfloat16))
    slot = rank + jnp.where(row >= rows, float(cap), 0.0)
    slot1 = jnp.where(picked > 0.0, slot + 1.0, 0.0).astype(jnp.bfloat16)
    rq = lax.broadcasted_iota(jnp.int32, (LANES, quota), 1)
    rn = lax.broadcasted_iota(jnp.int32, (LANES, quota), 0) * blk
    spread = jnp.where((rq >= rn) & (rq < rn + blk), 1.0, 0.0).astype(jnp.bfloat16)
    rep = dot(slot1, spread)
    qf = lax.broadcasted_iota(jnp.int32, (both, quota), 1).astype(jnp.float32)
    qslot = qf - jnp.floor((qf + 0.5) * (1.0 / blk)) * blk
    placing = jnp.where(rep == qslot + 1.0, 1.0, 0.0)
    place[...] = placing.astype(jnp.bfloat16)
    placing_t = jnp.transpose(placing).astype(jnp.bfloat16)

    qrow = lax.broadcasted_iota(jnp.int32, (quota, LANES), 0)
    qlane = lax.broadcasted_iota(jnp.int32, (quota, LANES), 1)
    ql = qlane * blk
    own_lane = (qrow >= ql) & (qrow < ql + blk)
    slot_gates = jnp.zeros((quota, LANES), jnp.float32)
    for e in range(per_node):
        g = jnp.zeros((both, LANES), jnp.float32)
        for k in range(k_top):
            hit = (f[:, k_sel + k : k_sel + k + 1] == nlane * per_node + e) & (lane < n)
            g = g + jnp.where(hit, f[:, k_sel + k_top + k : k_sel + k_top + k + 1], 0.0)
        picked_gate = dot(placing_t, g.astype(jnp.bfloat16))
        col = jnp.sum(jnp.where(own_lane, picked_gate, 0.0), axis=1, keepdims=True)
        slot_gates = jnp.where(qlane == e, col, slot_gates)
    packed[:, half:] = slot_gates.astype(jnp.bfloat16)

    tok_copy.wait()

    def pack(j, carry):
        cols = pl.ds(pl.multiple_of(j * chunk, LANES), chunk)
        packed[:, cols] = dot(placing_t, toks[:, cols]).astype(jnp.bfloat16)
        return carry

    lax.fori_loop(0, half // chunk, pack, 0)

    def a_copy(s):
        g, j = s // gs, s % gs
        return remote(
            packed.at[pl.ds(s * blk, blk)], rx.at[g, pl.ds(j * blk, blk)],
            a_send.at[s], a_recv.at[s], (partner(node, s, bits), loc),
        )

    for s in range(1, n):
        a_copy(s).start()
    rx[0, :blk, :] = packed[:blk, :]

    def y_copy(g):
        return remote(rx.at[g, pl.ds(0, gh)], rx.at[g, pl.ds(gh, gh)], y_send.at[g], y_recv.at[g], hi_peer)

    def d_copy(g, k):
        part = pl.ds(k * gh, gh)
        return remote(
            rx.at[g, part, pl.ds(0, half)], px.at[g, part],
            d_send.at[2 * g + k], d_recv.at[2 * g + k], lo_peer,
        )

    def fwd(g):
        for s in range(max(1, g * gs), (g + 1) * gs):
            a_copy(s).wait_recv()
        y_copy(g).start()
        d_copy(g, 0).start()

    def rel(g):
        y_copy(g).wait_recv()
        d_copy(g, 1).start()

    def e_copy(g):
        return remote(p_oth.at[g], pr.at[g], e_send.at[g], e_recv.at[g], lo_peer)

    def c_copy(g):
        return remote(p_own.at[g, pl.ds(gh, gh)], yr.at[g], c_send.at[g], c_recv.at[g], hi_peer)

    def b_copy(s):
        g, j = s // gs, s % gs
        return remote(
            p_own.at[g, pl.ds(j * blk, blk)], back.at[pl.ds(s * blk, blk)],
            b_send.at[s], b_recv.at[s], (partner(node, s, bits), loc),
        )

    glane = lax.broadcasted_iota(jnp.int32, (2 * gh, LANES), 1)

    def compute(g):
        d_copy(g, 0).wait_recv()
        d_copy(g, 1).wait_recv()
        gates = rx[g, :, half:].astype(jnp.float32)
        my_k = pl.ds(pl.multiple_of(lo * half, LANES), half)
        peer_k = pl.ds(pl.multiple_of((1 - lo) * half, LANES), half)

        def one(e, carry):
            lifted = dot(rx[g, :, :half], up[e, my_k, :]) + dot(px[g], up[e, peer_k, :])
            gate = jnp.sum(jnp.where(glane == e, gates, 0.0), axis=1, keepdims=True)
            scaled = lifted / (1.0 + jnp.exp(-lifted)) * gate
            hid[:, pl.ds(pl.multiple_of(e * unit, LANES), unit)] = scaled.astype(jnp.bfloat16)
            return carry

        lax.fori_loop(0, per_node, one, 0)

    def lower(g, dst, base):
        def one(j, carry):
            src = pl.ds(pl.multiple_of(base + j * chunk, LANES), chunk)
            cols = pl.ds(pl.multiple_of(j * chunk, LANES), chunk)
            dst[g, :, cols] = dot(hid[...], down[:, src]).astype(jnp.bfloat16)
            return carry

        lax.fori_loop(0, half // chunk, one, 0)

    def project(g):
        lower(g, p_oth, (1 - lo) * half)
        e_copy(g).start()
        lower(g, p_own, lo * half)

    def add_into(dst, g, part, src):
        def one(j, carry):
            cols = pl.ds(pl.multiple_of(j * chunk, LANES), chunk)
            total = dst[g, part, cols].astype(jnp.float32) + src[g, part, cols].astype(jnp.float32)
            dst[g, part, cols] = total.astype(jnp.bfloat16)
            return carry

        lax.fori_loop(0, half // chunk, one, 0)

    def comb1(g):
        e_copy(g).wait_recv()
        add_into(p_own, g, slice(gh, 2 * gh), pr)
        c_copy(g).start()
        add_into(p_own, g, slice(0, gh), pr)

    def comb2(g):
        c_copy(g).wait_recv()
        add_into(p_own, g, slice(0, gh), yr)
        for s in range(max(1, g * gs), (g + 1) * gs):
            b_copy(s).start()
        if g == 0:
            back[:blk, :] = p_own[0, :blk, :]

    fwd(0)
    fwd(1)
    rel(0)
    rel(1)
    up_copy.wait()
    down_copy.wait()
    fwd(2)
    compute(1)
    project(1)
    comb1(1)
    fwd(3)
    rel(2)
    compute(2)
    project(2)
    comb2(1)
    comb1(2)
    rel(3)
    compute(3)
    project(3)
    comb2(2)
    comb1(3)
    compute(0)
    project(0)
    comb1(0)
    comb2(3)
    comb2(0)

    for s in range(1, n):
        b_copy(s).wait_recv()

    def merge(j, carry):
        cols = pl.ds(pl.multiple_of(j * chunk, LANES), chunk)
        final[:, cols] = dot(place[...], back[:, cols]).astype(jnp.bfloat16)
        return carry

    lax.fori_loop(0, half // chunk, merge, 0)
    theirs = pl.ds(pl.multiple_of((1 - lo) * rows, rows), rows)
    f_copy = remote(final.at[theirs], out_ref.at[:, my_cols], f_send.at[0], f_recv.at[0], lo_peer)
    f_copy.start()
    out_ref[:, my_cols] = final[mine, :]

    for s in range(1, n):
        a_copy(s).wait_send()
        b_copy(s).wait_send()
    for g in range(GROUPS):
        y_copy(g).wait_send()
        d_copy(g, 0).wait_send()
        d_copy(g, 1).wait_send()
        e_copy(g).wait_send()
        c_copy(g).wait_send()
    f_copy.wait()


def body(tokens, node_ids, expert_ids, gate_weights, up_weight, down_weight):
    rows, model_width = tokens.shape
    n = lax.axis_size("node")
    per_node, _, unit = up_weight.shape
    cap = node_ids.shape[1] * rows // n
    blk = -(-2 * cap // 16) * 16
    half = model_width // 2
    width = half + LANES
    bits = n.bit_length() - 1
    chunk = next(c for c in (512, 256, 128) if half % c == 0)
    gs = n // GROUPS
    gr = 2 * gs * blk
    cfg = (n, bits, cap, blk, rows, half, width, per_node, unit, chunk)
    bf = jnp.bfloat16
    dma = pltpu.SemaphoreType.DMA
    vmem = pl.BlockSpec(memory_space=pltpu.VMEM)
    hbm = pl.BlockSpec(memory_space=pl.ANY)
    return pl.pallas_call(
        functools.partial(kernel, cfg),
        out_shape=jax.ShapeDtypeStruct((rows, model_width), bf),
        in_specs=[vmem, vmem, vmem, vmem, hbm, hbm],
        out_specs=vmem,
        scratch_shapes=[
            pltpu.VMEM(up_weight.shape, bf),
            pltpu.VMEM((per_node * unit, model_width), bf),
            pltpu.VMEM((2 * rows, half), bf),
            pltpu.VMEM((2 * rows, LANES), bf),
            pltpu.VMEM((rows, LANES), bf),
            pltpu.VMEM((n * blk, width), bf),
            pltpu.VMEM((GROUPS, gr, width), bf),
            pltpu.VMEM((GROUPS, gr, half), bf),
            pltpu.VMEM((gr, per_node * unit), bf),
            pltpu.VMEM((GROUPS, gr, half), bf),
            pltpu.VMEM((GROUPS, gr, half), bf),
            pltpu.VMEM((GROUPS, gr, half), bf),
            pltpu.VMEM((GROUPS, gr // 2, half), bf),
            pltpu.VMEM((n * blk, half), bf),
            pltpu.VMEM((2 * rows, n * blk), bf),
            pltpu.VMEM((2 * rows, half), bf),
            dma((2,)),
            dma((2,)), dma((2,)),
            dma((n,)), dma((n,)),
            dma((GROUPS,)), dma((GROUPS,)),
            dma((2 * GROUPS,)), dma((2 * GROUPS,)),
            dma((GROUPS,)), dma((GROUPS,)),
            dma((GROUPS,)), dma((GROUPS,)),
            dma((n,)), dma((n,)),
            dma((1,)), dma((1,)),
        ],
        compiler_params=pltpu.CompilerParams(
            collective_id=0, has_side_effects=True, vmem_limit_bytes=67043328
        ),
    )(
        tokens, node_ids, expert_ids, gate_weights, up_weight,
        down_weight.reshape(per_node * unit, model_width),
    )


def solution(mesh):
    in_specs = (
        P(("node", "local"), None),
        P(("node", "local"), None),
        P(("node", "local"), None),
        P(("node", "local"), None),
        P("node", None, "local"),
        P("node", "local", None),
    )
    out_specs = P(("node", "local"), None)
    return jax.shard_map(body, mesh=mesh, in_specs=in_specs, out_specs=out_specs, check_vma=False)
```

```python
import functools

import jax
import jax.numpy as jnp
from jax import lax
from jax.experimental import pallas as pl
from jax.experimental.pallas import tpu as pltpu
from jax.sharding import PartitionSpec as P

GROUPS = 4
LANES = 128
MESH = pl.DeviceIdType.MESH


def partner(index, step, bits):
    total = 0
    for b in range(bits):
        w = 1 << b
        total = total + ((index // w + step // w) % 2) * w
    return total


def dot(a, b):
    return jnp.dot(a, b, preferred_element_type=jnp.float32)


def kernel(
    cfg,
    tok_ref, nid_ref, eid_ref, gate_ref, up_hbm, down_hbm,
    out_ref,
    up, down, toks, ext, ext_own, packed, rx, px, hid, p_own, p_oth, pr, yr, back, place, final,
    w_sem, x_send, x_recv, a_send, a_recv, y_send, y_recv, d_send, d_recv,
    e_send, e_recv, c_send, c_recv, b_send, b_recv, f_send, f_recv,
):
    n, bits, cap, blk, rows, half, width, per_node, unit, chunk = cfg
    gs = n // GROUPS
    gh = gs * blk
    hb = gs // 2
    uh = hb * blk
    quota = n * blk
    node = lax.axis_index("node")
    loc = lax.axis_index("local")
    hi, lo = loc // 2, loc % 2
    lo_peer = (node, hi * 2 + (1 - lo))
    hi_peer = (node, (1 - hi) * 2 + lo)

    def remote(src, dst, ssem, rsem, dev):
        return pltpu.make_async_remote_copy(
            src_ref=src, dst_ref=dst, send_sem=ssem, recv_sem=rsem,
            device_id=dev, device_id_type=MESH,
        )

    up_copy = pltpu.make_async_copy(up_hbm, up, w_sem.at[0])
    down_copy = pltpu.make_async_copy(down_hbm, down, w_sem.at[1])
    up_copy.start()
    down_copy.start()

    barrier = pltpu.get_barrier_semaphore()
    for s in range(1, n):
        pl.semaphore_signal(barrier, inc=1, device_id=(partner(node, s, bits), loc), device_id_type=MESH)
    pl.semaphore_signal(barrier, inc=1, device_id=lo_peer, device_id_type=MESH)
    pl.semaphore_signal(barrier, inc=1, device_id=hi_peer, device_id_type=MESH)

    k_sel = nid_ref.shape[0]
    k_top = eid_ref.shape[0]
    line = lax.broadcasted_iota(jnp.int32, (LANES, rows), 0)
    facts = jnp.zeros((LANES, rows), jnp.float32)
    nid = nid_ref[...].astype(jnp.float32)
    eid = eid_ref[...].astype(jnp.float32)
    gat = gate_ref[...].astype(jnp.float32)
    for j in range(k_sel):
        facts = jnp.where(line == j, nid[j : j + 1, :], facts)
    for j in range(k_top):
        facts = jnp.where(line == k_sel + j, eid[j : j + 1, :], facts)
        facts = jnp.where(line == k_sel + k_top + j, gat[j : j + 1, :], facts)
    facts = jnp.transpose(facts)
    mine = pl.ds(pl.multiple_of(lo * rows, rows), rows)
    ext_own[...] = facts.astype(jnp.bfloat16)
    my_cols = pl.ds(pl.multiple_of(lo * half, LANES), half)
    peer_cols = pl.ds(pl.multiple_of((1 - lo) * half, LANES), half)

    pl.semaphore_wait(barrier, n + 1)
    ext_copy = remote(ext_own, ext.at[mine], x_send.at[0], x_recv.at[0], lo_peer)
    ext_copy.start()
    tok_copy = remote(tok_ref.at[:, peer_cols], toks.at[mine], x_send.at[1], x_recv.at[1], lo_peer)
    tok_copy.start()
    ext[mine, :] = facts.astype(jnp.bfloat16)
    toks[mine, :] = tok_ref[:, my_cols]
    ext_copy.wait()

    both = 2 * rows
    f = ext[...].astype(jnp.float32)
    lane = lax.broadcasted_iota(jnp.int32, (both, LANES), 1)
    row = lax.broadcasted_iota(jnp.int32, (both, LANES), 0)
    nlane = jnp.where(lane < n, jnp.bitwise_xor(lane, node), -1).astype(jnp.float32)
    picked = jnp.zeros((both, LANES), jnp.float32)
    for j in range(k_sel):
        picked = picked + jnp.where(f[:, j : j + 1] == nlane, 1.0, 0.0)
    tr = lax.broadcasted_iota(jnp.int32, (both, both), 0)
    tc = lax.broadcasted_iota(jnp.int32, (both, both), 1)
    earlier = jnp.where((tc < tr) & ((tc >= rows) == (tr >= rows)), 1.0, 0.0).astype(jnp.bfloat16)
    rank = dot(earlier, picked.astype(jnp.bfloat16))
    slot = rank + jnp.where(row >= rows, float(cap), 0.0)
    slot1 = jnp.where(picked > 0.0, slot + 1.0, 0.0).astype(jnp.bfloat16)
    rq = lax.broadcasted_iota(jnp.int32, (LANES, quota), 1)
    rn = lax.broadcasted_iota(jnp.int32, (LANES, quota), 0) * blk
    spread = jnp.where((rq >= rn) & (rq < rn + blk), 1.0, 0.0).astype(jnp.bfloat16)
    rep = dot(slot1, spread)
    qf = lax.broadcasted_iota(jnp.int32, (both, quota), 1).astype(jnp.float32)
    qslot = qf - jnp.floor((qf + 0.5) * (1.0 / blk)) * blk
    placing = jnp.where(rep == qslot + 1.0, 1.0, 0.0)
    place[...] = placing.astype(jnp.bfloat16)
    placing_t = jnp.transpose(placing).astype(jnp.bfloat16)

    qrow = lax.broadcasted_iota(jnp.int32, (quota, LANES), 0)
    qlane = lax.broadcasted_iota(jnp.int32, (quota, LANES), 1)
    ql = qlane * blk
    own_lane = (qrow >= ql) & (qrow < ql + blk)
    slot_gates = jnp.zeros((quota, LANES), jnp.float32)
    for e in range(per_node):
        g = jnp.zeros((both, LANES), jnp.float32)
        for k in range(k_top):
            hit = (f[:, k_sel + k : k_sel + k + 1] == nlane * per_node + e) & (lane < n)
            g = g + jnp.where(hit, f[:, k_sel + k_top + k : k_sel + k_top + k + 1], 0.0)
        picked_gate = dot(placing_t, g.astype(jnp.bfloat16))
        col = jnp.sum(jnp.where(own_lane, picked_gate, 0.0), axis=1, keepdims=True)
        slot_gates = jnp.where(qlane == e, col, slot_gates)
    packed[:, half:] = slot_gates.astype(jnp.bfloat16)

    tok_copy.wait()

    def pack(j, carry):
        cols = pl.ds(pl.multiple_of(j * chunk, LANES), chunk)
        packed[:, cols] = dot(placing_t, toks[:, cols]).astype(jnp.bfloat16)
        return carry

    lax.fori_loop(0, half // chunk, pack, 0)

    def a_copy(s):
        g, j = s // gs, s % gs
        return remote(
            packed.at[pl.ds(s * blk, blk)], rx.at[g, pl.ds(j * blk, blk)],
            a_send.at[s], a_recv.at[s], (partner(node, s, bits), loc),
        )

    for s in range(1, n // 2):
        a_copy(s).start()
        a_copy(s + n // 2 - 1).start()
    a_copy(n - 1).start()
    rx[0, :blk, :] = packed[:blk, :]

    def y_copy(u):
        g, base = u // 2, (u % 2) * uh
        return remote(
            rx.at[g, pl.ds(base, uh)], rx.at[g, pl.ds(gh + base, uh)],
            y_send.at[u], y_recv.at[u], hi_peer,
        )

    def d_copy(g, k):
        part = pl.ds(k * gh, gh)
        return remote(
            rx.at[g, part, pl.ds(0, half)], px.at[g, part],
            d_send.at[2 * g + k], d_recv.at[2 * g + k], lo_peer,
        )

    def fwd(u):
        for s in range(max(1, u * hb), (u + 1) * hb):
            a_copy(s).wait_recv()
        y_copy(u).start()
        if u % 2:
            d_copy(u // 2, 0).start()

    def rel(g):
        y_copy(2 * g).wait_recv()
        y_copy(2 * g + 1).wait_recv()
        d_copy(g, 1).start()

    def e_copy(g):
        return remote(p_oth.at[g], pr.at[g], e_send.at[g], e_recv.at[g], lo_peer)

    def c_copy(u):
        g, base = u // 2, (u % 2) * uh
        return remote(
            p_own.at[g, pl.ds(gh + base, uh)], yr.at[g, pl.ds(base, uh)],
            c_send.at[u], c_recv.at[u], hi_peer,
        )

    def b_copy(s):
        g, j = s // gs, s % gs
        return remote(
            p_own.at[g, pl.ds(j * blk, blk)], back.at[pl.ds(s * blk, blk)],
            b_send.at[s], b_recv.at[s], (partner(node, s, bits), loc),
        )

    glane = lax.broadcasted_iota(jnp.int32, (2 * gh, LANES), 1)

    def compute(g):
        d_copy(g, 0).wait_recv()
        d_copy(g, 1).wait_recv()
        gates = rx[g, :, half:].astype(jnp.float32)
        my_k = pl.ds(pl.multiple_of(lo * half, LANES), half)
        peer_k = pl.ds(pl.multiple_of((1 - lo) * half, LANES), half)

        def one(e, carry):
            lifted = dot(rx[g, :, :half], up[e, my_k, :]) + dot(px[g], up[e, peer_k, :])
            gate = jnp.sum(jnp.where(glane == e, gates, 0.0), axis=1, keepdims=True)
            scaled = lifted / (1.0 + jnp.exp(-lifted)) * gate
            hid[:, pl.ds(pl.multiple_of(e * unit, LANES), unit)] = scaled.astype(jnp.bfloat16)
            return carry

        lax.fori_loop(0, per_node, one, 0)

    def lower(g, dst, base):
        def one(j, carry):
            src = pl.ds(pl.multiple_of(base + j * chunk, LANES), chunk)
            cols = pl.ds(pl.multiple_of(j * chunk, LANES), chunk)
            dst[g, :, cols] = dot(hid[...], down[:, src]).astype(jnp.bfloat16)
            return carry

        lax.fori_loop(0, half // chunk, one, 0)

    def project(g):
        lower(g, p_oth, (1 - lo) * half)
        e_copy(g).start()
        lower(g, p_own, lo * half)

    def add_into(g, part, *others):
        def one(j, carry):
            cols = pl.ds(pl.multiple_of(j * chunk, LANES), chunk)
            total = p_own[g, part, cols].astype(jnp.float32)
            for other in others:
                total = total + other[g, part, cols].astype(jnp.float32)
            p_own[g, part, cols] = total.astype(jnp.bfloat16)
            return carry

        lax.fori_loop(0, half // chunk, one, 0)

    def comb1(u):
        base = gh + (u % 2) * uh
        add_into(u // 2, slice(base, base + uh), pr)
        c_copy(u).start()

    def comb2(u):
        base = (u % 2) * uh
        c_copy(u).wait_recv()
        add_into(u // 2, slice(base, base + uh), pr, yr)
        for s in range(max(1, u * hb), (u + 1) * hb):
            b_copy(s).start()
        if u == 0:
            back[:blk, :] = p_own[0, :blk, :]

    fwd(0)
    fwd(1)
    fwd(2)
    fwd(3)
    rel(0)
    up_copy.wait()
    down_copy.wait()
    compute(0)
    fwd(4)
    project(0)
    fwd(5)
    rel(1)
    compute(1)
    project(1)
    fwd(6)
    e_copy(1).wait_recv()
    comb1(2)
    rel(2)
    compute(2)
    project(2)
    e_copy(2).wait_recv()
    comb1(4)
    fwd(7)
    comb1(5)
    comb2(2)
    comb2(4)
    rel(3)
    compute(3)
    comb2(5)
    project(3)
    e_copy(3).wait_recv()
    comb1(6)
    comb1(7)
    comb1(3)
    e_copy(0).wait_recv()
    comb1(1)
    comb1(0)
    comb2(6)
    comb2(7)
    comb2(3)
    comb2(1)
    comb2(0)

    for s in range(1, n):
        b_copy(s).wait_recv()

    def merge(j, carry):
        cols = pl.ds(pl.multiple_of(j * chunk, LANES), chunk)
        final[:, cols] = dot(place[...], back[:, cols]).astype(jnp.bfloat16)
        return carry

    lax.fori_loop(0, half // chunk, merge, 0)
    theirs = pl.ds(pl.multiple_of((1 - lo) * rows, rows), rows)
    f_copy = remote(final.at[theirs], out_ref.at[:, my_cols], f_send.at[0], f_recv.at[0], lo_peer)
    f_copy.start()
    out_ref[:, my_cols] = final[mine, :]

    for s in range(1, n):
        a_copy(s).wait_send()
        b_copy(s).wait_send()
    for g in range(GROUPS):
        y_copy(2 * g).wait_send()
        y_copy(2 * g + 1).wait_send()
        c_copy(2 * g).wait_send()
        c_copy(2 * g + 1).wait_send()
        d_copy(g, 0).wait_send()
        d_copy(g, 1).wait_send()
        e_copy(g).wait_send()
    f_copy.wait()


def body(tokens, node_ids, expert_ids, gate_weights, up_weight, down_weight):
    rows, model_width = tokens.shape
    n = lax.axis_size("node")
    per_node, _, unit = up_weight.shape
    cap = node_ids.shape[1] * rows // n
    blk = -(-2 * cap // 16) * 16
    half = model_width // 2
    width = half + LANES
    bits = n.bit_length() - 1
    chunk = next(c for c in (512, 256, 128) if half % c == 0)
    gs = n // GROUPS
    gr = 2 * gs * blk
    cfg = (n, bits, cap, blk, rows, half, width, per_node, unit, chunk)
    bf = jnp.bfloat16
    dma = pltpu.SemaphoreType.DMA
    vmem = pl.BlockSpec(memory_space=pltpu.VMEM)
    hbm = pl.BlockSpec(memory_space=pl.ANY)
    return pl.pallas_call(
        functools.partial(kernel, cfg),
        out_shape=jax.ShapeDtypeStruct((rows, model_width), bf),
        in_specs=[vmem, vmem, vmem, vmem, hbm, hbm],
        out_specs=vmem,
        scratch_shapes=[
            pltpu.VMEM(up_weight.shape, bf),
            pltpu.VMEM((per_node * unit, model_width), bf),
            pltpu.VMEM((2 * rows, half), bf),
            pltpu.VMEM((2 * rows, LANES), bf),
            pltpu.VMEM((rows, LANES), bf),
            pltpu.VMEM((n * blk, width), bf),
            pltpu.VMEM((GROUPS, gr, width), bf),
            pltpu.VMEM((GROUPS, gr, half), bf),
            pltpu.VMEM((gr, per_node * unit), bf),
            pltpu.VMEM((GROUPS, gr, half), bf),
            pltpu.VMEM((GROUPS, gr, half), bf),
            pltpu.VMEM((GROUPS, gr, half), bf),
            pltpu.VMEM((GROUPS, gr // 2, half), bf),
            pltpu.VMEM((n * blk, half), bf),
            pltpu.VMEM((2 * rows, n * blk), bf),
            pltpu.VMEM((2 * rows, half), bf),
            dma((2,)),
            dma((2,)), dma((2,)),
            dma((n,)), dma((n,)),
            dma((2 * GROUPS,)), dma((2 * GROUPS,)),
            dma((2 * GROUPS,)), dma((2 * GROUPS,)),
            dma((GROUPS,)), dma((GROUPS,)),
            dma((2 * GROUPS,)), dma((2 * GROUPS,)),
            dma((n,)), dma((n,)),
            dma((1,)), dma((1,)),
        ],
        compiler_params=pltpu.CompilerParams(
            collective_id=0, has_side_effects=True, vmem_limit_bytes=67043328
        ),
    )(
        tokens, node_ids.T, expert_ids.T, gate_weights.T, up_weight,
        down_weight.reshape(per_node * unit, model_width),
    )


def solution(mesh):
    in_specs = (
        P(("node", "local"), None),
        P(("node", "local"), None),
        P(("node", "local"), None),
        P(("node", "local"), None),
        P("node", None, "local"),
        P("node", "local", None),
    )
    out_specs = P(("node", "local"), None)
    return jax.shard_map(body, mesh=mesh, in_specs=in_specs, out_specs=out_specs, check_vma=False)
```
